32 devices in a mesh: gx: 4 (over y, x), gy: 2 (over core), gz: 4 (over z).
Axes of the slice: x: 2, y: 2, z: 4, core: 2. Of those that a mesh axis runs over, the one named last changes fastest.
Arguments:
- rhs: float32 [8, 64, 64, 512], P(None, 'gx', 'gy', 'gz'), may hold values from -8 to 8
- stencil: float32 [14, 64, 64, 512], P(None, 'gx', 'gy', 'gz'), may hold values from 0.02 to 1
Outputs:
- solution: float32 [8, 64, 64, 512], P(None, 'gx', 'gy', 'gz')
- residual: float32 [8, 64, 64, 512], P(None, 'gx', 'gy', 'gz')
The draws below stay inside these ranges and needn't reach their ends.
All inputs are finite; a program needn't handle non-finite values.
Results may differ from the reference program's by a relative error of at most 0.00029.
Values sent between devices are 32-bit elements; how exact they have to be, the bound alone decides.
A program may use at most 128 MiB of HBM per device.

```python
import math
import jax
import jax.numpy as jnp
from jax import lax

NRHS = 8
ITERS = 2
NX = 64
NY = 64
NZ = 512


def block_levels(own_key, dims, shards, low, high):
    level = 1.0
    for dim, blocks in shards:
        steps = jax.random.uniform(jax.random.fold_in(jax.random.fold_in(own_key, 6), dim), (blocks,), jnp.float32, low / len(shards), high / len(shards))
        level = level * jnp.repeat(jnp.exp(steps), dims[dim] // blocks).reshape((-1,) + (1,) * (len(dims) - 1 - dim))
    return level


def bell_draw(rng, shape, scale, bound, split=(), dtype=jnp.bfloat16):
    level = block_levels(rng, shape, split, -0.22, 0.18) if split else 1.0
    values = jax.random.normal(rng, shape, jnp.float32) * scale * level
    return jnp.minimum(jnp.maximum(values, -bound), bound).astype(dtype)


def setup_inputs(seed: int = 0) -> dict:
    seeds = jax.random.split(jax.random.key(seed), 3)
    return {
        "rhs": bell_draw(seeds[0], (NRHS, NX, NY, NZ), 1.0, 8.0, ((1, 4), (2, 2), (3, 4)), jnp.float32),
        "stencil": jnp.clip(jnp.exp(math.log(1.0) - 3.912023 * jax.random.uniform(seeds[1], (14, NX, NY, NZ), jnp.float32) ** block_levels(seeds[1], (14, NX, NY, NZ), ((1, 4), (2, 2), (3, 4)), -0.2, 0.2)), 0.02, 1.0),
    }


FORWARD = [(a, b, c) for a in (-1, 0, 1) for b in (-1, 0, 1) for c in (-1, 0, 1) if (a, b, c) > (0, 0, 0)]

def window(array, margin, depth, offset):
    result = array
    for place in range(3):
        dim = array.ndim - 3 + place
        inner = array.shape[dim] - 2 * margin
        begin = margin - depth + offset[place]
        result = lax.slice_in_dim(result, begin, begin + inner + 2 * depth, axis=dim)
    return result

def diagonal_field(padded, margin, depth):
    total = window(padded[0], margin, depth, (0, 0, 0))
    total = total + jnp.sum(window(padded[1:], margin, depth, (0, 0, 0)), axis=0)
    for index, offset in enumerate(FORWARD):
        back = (-offset[0], -offset[1], -offset[2])
        total = total + window(padded[index + 1], margin, depth, back)
    return total

def operate(field, fmargin, padded, smargin, diag, depth):
    result = diag[None] * window(field, fmargin, depth, (0, 0, 0))
    for index, offset in enumerate(FORWARD):
        back = (-offset[0], -offset[1], -offset[2])
        ahead_w = window(padded[index + 1], smargin, depth, (0, 0, 0))
        behind_w = window(padded[index + 1], smargin, depth, back)
        result = result - ahead_w[None] * window(field, fmargin, depth, offset)
        result = result - behind_w[None] * window(field, fmargin, depth, back)
    return result

def gram(left, right):
    flat_l = left.reshape(left.shape[0], -1)
    flat_r = right.reshape(right.shape[0], -1)
    return lax.dot_general(flat_l.astype(jnp.float32), flat_r.astype(jnp.float32), (((1,), (1,)), ((), ())), precision=lax.Precision.HIGHEST, preferred_element_type=jnp.float32)

def combine(coef, field):
    return jnp.einsum('ij,ixyz->jxyz', coef, field, precision=lax.Precision.HIGHEST)

def solve_spd(matrix, right):
    factor = jnp.linalg.cholesky(matrix)
    return jax.scipy.linalg.cho_solve((factor, True), right)

def reference(rhs, stencil):
    padded = jnp.pad(stencil, ((0, 0), (1, 1), (1, 1), (1, 1)))
    diag = diagonal_field(padded, 1, 0)
    solution = jnp.zeros_like(rhs)
    residual = rhs
    direction = rhs
    norm_now = gram(residual, residual)
    for step in range(ITERS):
        field = jnp.pad(direction, ((0, 0), (1, 1), (1, 1), (1, 1)))
        image = operate(field, 1, padded, 1, diag, 0)
        alpha = solve_spd(gram(direction, image), norm_now)
        solution = solution + combine(alpha, direction)
        residual = residual - combine(alpha, image)
        if step + 1 < ITERS:
            norm_next = gram(residual, residual)
            beta = solve_spd(norm_now, norm_next)
            direction = residual + combine(beta, direction)
            norm_now = norm_next
    return (solution, residual)
```

```python
import jax
import jax.numpy as jnp
from jax import lax
from jax.experimental import pallas as pl
from jax.experimental.pallas import tpu as pltpu
from jax.sharding import PartitionSpec as P

FORWARD = [
    (a, b, c) for a in (-1, 0, 1) for b in (-1, 0, 1) for c in (-1, 0, 1) if (a, b, c) > (0, 0, 0)
]
AXES = ("gx", "gy", "gz")
LO = [k for k, o in enumerate(FORWARD) if o[2] == 1]
HI = [k for k, o in enumerate(FORWARD) if o[2] == -1]
EX = [k for k, o in enumerate(FORWARD) if o[0] == 1]
F32 = jnp.float32


def runs(ks):
    out = []
    for k in ks:
        if out and out[-1][1] == k:
            out[-1][1] = k + 1
        else:
            out.append([k, k + 1])
    return out


def mm(a, b):
    total = a[:, 0:1] * b[0:1, :]
    for k in range(1, 8):
        total = total + a[:, k : k + 1] * b[k : k + 1, :]
    return total


def solve(matrix, right, row):
    aug = matrix + pltpu.roll(right, 8, 1)
    for k in range(8):
        pivot = aug[k : k + 1, :] / aug[k : k + 1, k : k + 1]
        aug = jnp.where(row == k, pivot, aug - aug[:, k : k + 1] * pivot)
    return pltpu.roll(aug, 120, 1)


def transposed(a, row, lane):
    out = jnp.zeros_like(a)
    for i in range(8):
        line = jnp.sum(jnp.where(lane == row, a[:, i : i + 1], 0.0), axis=0, keepdims=True)
        out = out + jnp.where(row == i, line, 0.0)
    return out


def main_kernel(sizes, dims, rhs, sten, q1_out, q2_out, c_out, p0, q0, pm, pp, w, ws, s0, diag, q2,
                zsend, zrecv, wzsend, wzrecv, red, gacc, cur, slot_x, slot_y, slot_z, lsem,
                xs, xr, ars, arr):
    nf, nx, ny = dims
    yb_n = ny // 8
    tall = ny + 16
    tiles = tall // 8
    pos = {a: lax.axis_index(a) for a in AXES}
    lane = lax.broadcasted_iota(jnp.int32, (8, 128), 1)
    row = lax.broadcasted_iota(jnp.int32, (8, 128), 0)
    ys = pl.ds(8, ny)

    loads = [
        pltpu.make_async_copy(rhs, p0.at[:, pl.ds(1, nx), ys], lsem.at[0]),
        pltpu.make_async_copy(sten.at[pl.ds(1, 13)], w.at[:, pl.ds(1, nx), ys], lsem.at[1]),
        pltpu.make_async_copy(sten.at[0], s0, lsem.at[2]),
    ]
    for copy in loads:
        copy.start()

    for buf in (p0, q0):
        for x in (0, nx + 1):
            buf[:, x] = jnp.zeros((nf, tall, 128), F32)
    w[:, 0] = jnp.zeros((13, tall, 128), F32)

    def clear(x, carry):
        for y in (0, ny + 8):
            p0[:, x, y : y + 8] = jnp.zeros((nf, 8, 128), F32)
            q0[:, x, y : y + 8] = jnp.zeros((nf, 8, 128), F32)
            w[:, x, y : y + 8] = jnp.zeros((13, 8, 128), F32)
        return carry

    lax.fori_loop(1, nx + 1, clear, 0)
    zrecv[...] = jnp.zeros(zrecv.shape, F32)
    wzrecv[...] = jnp.zeros(wzrecv.shape, F32)

    barrier = pltpu.get_barrier_semaphore()
    for a in AXES:
        for d in range(1, sizes[a]):
            pl.semaphore_signal(barrier, inc=1, device_id={a: lax.rem(pos[a] + d, sizes[a])},
                                device_id_type=pl.DeviceIdType.MESH)
    pl.semaphore_wait(barrier, sum(sizes[a] - 1 for a in AXES))

    count = [0]

    def shift(axis, up, src, dst):
        n = sizes[axis]
        i = pos[axis]
        slot = count[0]
        count[0] += 1
        copy = pltpu.make_async_remote_copy(
            src_ref=src, dst_ref=dst, send_sem=xs.at[slot], recv_sem=xr.at[slot],
            device_id={axis: lax.rem(i + (1 if up else n - 1), n)},
            device_id_type=pl.DeviceIdType.MESH)
        sends = i < n - 1 if up else i > 0
        gets = i > 0 if up else i < n - 1

        @pl.when(sends)
        def _():
            copy.start()

        def finish():
            @pl.when(sends)
            def _():
                copy.wait_send()

            @pl.when(gets)
            def _():
                copy.wait_recv()

        return finish

    def finish_all(items):
        for f in items:
            f()

    def y_faces(buf):
        return [
            shift("gy", True, buf.at[:, :, pl.ds(ny, 8)], buf.at[:, :, pl.ds(0, 8)]),
            shift("gy", False, buf.at[:, :, pl.ds(8, 8)], buf.at[:, :, pl.ds(ny + 8, 8)]),
        ]

    def pack(buf, depth, first, which):
        n = len(which)

        def take(k_x, yb):
            if which is ALL:
                return buf[:, k_x, yb * 8 : yb * 8 + 8]
            return jnp.concatenate([buf[k : k + 1, k_x, yb * 8 : yb * 8 + 8] for k in which], axis=0)

        def body(x, acc):
            for yb in range(tiles):
                j = x * tiles + yb
                v = pltpu.roll(take(x, yb), lax.rem(j + 128 - first, 128), 2)
                acc = jnp.where((lane == j)[None], v, acc)
            return acc

        return lax.fori_loop(0, depth, body, jnp.zeros((n, 8, 128), F32))

    ALL = list(range(nf))

    def gram(g, u, v):
        def body(x, accs):
            accs = list(accs)
            for yb in range(yb_n):
                ub = u(x, yb)
                vb = v(x, yb)
                for i in range(nf):
                    accs[i] = accs[i] + ub[i : i + 1] * vb[i:]
            return tuple(accs)

        accs = lax.fori_loop(0, nx, body, tuple(jnp.zeros((nf - i, 8, 128), F32) for i in range(nf)))
        red[...] = jnp.zeros(red.shape, F32)
        for i in range(nf):
            red[i, i:nf, :] = jnp.sum(accs[i], axis=1)
        out = jnp.zeros((8, 128), F32)
        for i in range(nf):
            t = jnp.sum(red[i], axis=1, keepdims=True)
            out = out + jnp.where(lane == 8 * g + i, t, 0.0)
            line = jnp.sum(jnp.where(lane == 8 * g + row, t, 0.0), axis=0, keepdims=True)
            out = out + jnp.where((row == i) & (lane > 8 * g + i), line, 0.0)
        if g == 0:
            gacc[...] = out
        else:
            gacc[...] += out

    def own(buf):
        return lambda x, yb: buf[:, x + 1, 8 + yb * 8 : 16 + yb * 8]

    def z_send(buf, e):
        zsend[e, 0] = pack(buf, nx + 2, 127, ALL)
        zsend[e, 1] = pack(buf, nx + 2, 0, ALL)
        return [
            shift("gz", True, zsend.at[e, 0], zrecv.at[e, 0]),
            shift("gz", False, zsend.at[e, 1], zrecv.at[e, 1]),
        ]

    def z_fill(buf, e):
        def body(x, carry):
            for yb in range(tiles):
                j = x * tiles + yb
                v = buf[:, x, yb * 8 : yb * 8 + 8]
                low = pltpu.roll(zrecv[e, 0], lax.rem(128 - j, 128), 2)
                high = pltpu.roll(zrecv[e, 1], 127 - j, 2)
                pm[:, x, yb * 8 : yb * 8 + 8] = jnp.where((lane == 0)[None], low, pltpu.roll(v, 1, 2))
                pp[:, x, yb * 8 : yb * 8 + 8] = jnp.where((lane == 127)[None], high, pltpu.roll(v, 127, 2))
            return carry

        lax.fori_loop(0, nx + 2, body, 0)

    def behind(k, x, yb):
        a, b, c = FORWARD[k]
        src = w if c == 0 else ws
        return src[k, x + 1 - a, 8 + yb * 8 - b : 16 + yb * 8 - b]

    def ahead(k, x, yb):
        return w[k, x + 1, 8 + yb * 8 : 16 + yb * 8]

    def stencil(buf, put):
        views = {0: buf, -1: pm, 1: pp}

        def body(x, carry):
            for yb in range(yb_n):
                y = 8 + yb * 8
                acc = diag[x, yb * 8 : yb * 8 + 8][None] * buf[:, x + 1, y : y + 8]
                for k, (a, b, c) in enumerate(FORWARD):
                    acc = acc - ahead(k, x, yb)[None] * views[c][:, x + 1 + a, y + b : y + b + 8]
                    acc = acc - behind(k, x, yb)[None] * views[-c][:, x + 1 - a, y - b : y - b + 8]
                put(x, yb, acc)
            return carry

        lax.fori_loop(0, nx, body, 0)

    k0, k1 = EX[0], EX[-1] + 1
    phase = [
        shift("gx", True, rhs.at[:, nx - 1], p0.at[:, 0, ys]),
        shift("gx", False, rhs.at[:, 0], p0.at[:, nx + 1, ys]),
        shift("gx", True, sten.at[pl.ds(k0 + 1, k1 - k0), nx - 1], w.at[pl.ds(k0, k1 - k0), 0, ys]),
    ]
    loads[0].wait()
    gram(0, own(p0), own(p0))
    loads[1].wait()
    loads[2].wait()
    finish_all(phase)
    phase = y_faces(p0)
    for b, up, src, dst in ((1, True, ny, 0), (-1, False, 8, ny + 8)):
        for lo, hi in runs([k for k, o in enumerate(FORWARD) if o[1] == b]):
            ks = pl.ds(lo, hi - lo)
            phase.append(shift("gy", up, w.at[ks, :, pl.ds(src, 8)], w.at[ks, :, pl.ds(dst, 8)]))
    finish_all(phase)
    phase = z_send(p0, 0)
    wzsend[0 : len(LO)] = pack(w, nx + 1, 127, LO)
    wzsend[len(LO) : len(LO) + len(HI)] = pack(w, nx + 1, 0, HI)
    lo_part, hi_part = pl.ds(0, len(LO)), pl.ds(len(LO), len(HI))
    phase += [
        shift("gz", True, wzsend.at[lo_part], wzrecv.at[lo_part]),
        shift("gz", False, wzsend.at[hi_part], wzrecv.at[hi_part]),
    ]
    finish_all(phase)
    z_fill(p0, 0)

    def w_fill(x, carry):
        for yb in range(tiles):
            j = x * tiles + yb
            for n, k in enumerate(LO):
                v = pltpu.roll(w[k, x, yb * 8 : yb * 8 + 8], 1, 1)
                ws[k, x, yb * 8 : yb * 8 + 8] = jnp.where(
                    lane == 0, pltpu.roll(wzrecv[n], lax.rem(128 - j, 128), 1), v)
            for n, k in enumerate(HI):
                v = pltpu.roll(w[k, x, yb * 8 : yb * 8 + 8], 127, 1)
                ws[k, x, yb * 8 : yb * 8 + 8] = jnp.where(
                    lane == 127, pltpu.roll(wzrecv[len(LO) + n], 127 - j, 1), v)
        return carry

    lax.fori_loop(0, nx + 1, w_fill, 0)

    def make_diag(x, carry):
        for yb in range(yb_n):
            total = s0[x, yb * 8 : yb * 8 + 8]
            for k in range(13):
                total = total + ahead(k, x, yb) + behind(k, x, yb)
            diag[x, yb * 8 : yb * 8 + 8] = total
        return carry

    lax.fori_loop(0, nx, make_diag, 0)

    def put_q1(x, yb, v):
        q0[:, x + 1, 8 + yb * 8 : 16 + yb * 8] = v

    stencil(p0, put_q1)

    phase = [
        shift("gx", True, q0.at[:, nx, ys], q0.at[:, 0, ys]),
        shift("gx", False, q0.at[:, 1, ys], q0.at[:, nx + 1, ys]),
    ]
    save1 = pltpu.make_async_copy(q0.at[:, pl.ds(1, nx), ys], q1_out, lsem.at[3])
    save1.start()
    gram(1, own(p0), own(q0))
    finish_all(phase)
    phase = y_faces(q0)
    finish_all(phase)
    phase = z_send(q0, 1)
    gram(2, own(q0), own(q0))
    finish_all(phase)
    z_fill(q0, 1)

    def put_q2(x, yb, v):
        q2[:, x, yb * 8 : yb * 8 + 8] = v

    stencil(q0, put_q2)
    save2 = pltpu.make_async_copy(q2, q2_out, lsem.at[4])
    save2.start()
    gram(3, own(q0), lambda x, yb: q2[:, x, yb * 8 : yb * 8 + 8])

    total = gacc[...]
    base = 0
    for stage, (a, slots) in enumerate(zip(("gy", "gx", "gz"), (slot_y, slot_x, slot_z))):
        n = sizes[a]
        i = pos[a]
        cur[stage] = total
        slots[i] = total
        copies = []
        for d in range(1, n):
            copies.append(pltpu.make_async_remote_copy(
                src_ref=cur.at[stage], dst_ref=slots.at[i],
                send_sem=ars.at[base + d - 1], recv_sem=arr.at[base + d - 1],
                device_id={a: lax.rem(i + d, n)}, device_id_type=pl.DeviceIdType.MESH))
        for copy in copies:
            copy.start()
        for d, copy in zip(range(1, n), copies):
            copy.wait_send()
            pltpu.make_async_remote_copy(
                src_ref=cur.at[stage], dst_ref=slots.at[lax.rem(i + n - d, n)],
                send_sem=ars.at[base + d - 1], recv_sem=arr.at[base + d - 1],
                device_id={a: lax.rem(i + d, n)}, device_id_type=pl.DeviceIdType.MESH).wait_recv()
        total = slots[0]
        for s in range(1, n):
            total = total + slots[s]
        base += n - 1

    small = lane < 8
    parts = [jnp.where(small, pltpu.roll(total, (128 - 8 * g) % 128, 1), 0.0) for g in range(4)]
    rr, pq, ss, tt = parts
    alpha = jnp.where(small, solve(pq, rr, row), 0.0)
    alpha_t = transposed(alpha, row, lane)
    alpha_t = jnp.where(small, alpha_t, 0.0)
    ssa = mm(ss, alpha)
    new = rr - mm(alpha_t, pq) - mm(pq, alpha) + mm(alpha_t, ssa)
    beta = jnp.where(small, solve(rr, new, row), 0.0)
    ib = beta + jnp.where(lane == row, 1.0, 0.0)
    ib_t = jnp.where(small, transposed(ib, row, lane), 0.0)
    curve = mm(ib_t, mm(pq, ib) - ssa) - mm(alpha_t, mm(ss, ib) - mm(tt, alpha))
    alpha1 = jnp.where(small, solve(curve, new, row), 0.0)
    c_out[0] = alpha + mm(ib, alpha1)
    c_out[1] = mm(alpha, alpha1)
    save1.wait()
    save2.wait()


def final_kernel(yb_n, xs_n, c, r0, q1, q2, sol, res, table):
    @pl.when(pl.program_id(0) == 0)
    def _():
        for n in range(2):
            for i in range(8):
                for j in range(8):
                    table[n, i, j] = jnp.full((8, 128), c[n, i, j], F32)

    def body(x, carry):
        for yb in range(yb_n):
            y = slice(yb * 8, yb * 8 + 8)
            s = jnp.zeros((8, 8, 128), F32)
            e = r0[:, x, y]
            for i in range(8):
                t1, t2 = table[0, i], table[1, i]
                a, b, d = r0[i, x, y][None], q1[i, x, y][None], q2[i, x, y][None]
                s = s + (t1 * a - t2 * b)
                e = e + (t2 * d - t1 * b)
            sol[:, x, y] = s
            res[:, x, y] = e
        return carry

    lax.fori_loop(0, xs_n, body, 0)


def shards(sizes, rhs, stencil):
    nf, nx, ny, nz = rhs.shape
    tall = ny + 16
    field = jax.ShapeDtypeStruct(rhs.shape, F32)
    anyspace = pl.BlockSpec(memory_space=pl.ANY)
    peers = sum(sizes[a] - 1 for a in AXES)
    padded = pltpu.VMEM((nf, nx + 2, tall, nz), F32)

    def kernel(*refs):
        main_kernel(sizes, (nf, nx, ny), *refs)

    q1, q2, c = pl.pallas_call(
        kernel,
        out_shape=(field, field, jax.ShapeDtypeStruct((2, 8, 128), F32)),
        in_specs=[anyspace, anyspace],
        out_specs=(anyspace, anyspace, pl.BlockSpec(memory_space=pltpu.VMEM)),
        scratch_shapes=[
            padded, padded, padded, padded,
            pltpu.VMEM((13, nx + 1, tall, nz), F32),
            pltpu.VMEM((13, nx + 1, tall, nz), F32),
            pltpu.VMEM((nx, ny, nz), F32),
            pltpu.VMEM((nx, ny, nz), F32),
            pltpu.VMEM((nf, nx, ny, nz), F32),
            pltpu.VMEM((2, 2, nf, 8, nz), F32),
            pltpu.VMEM((2, 2, nf, 8, nz), F32),
            pltpu.VMEM((len(LO) + len(HI), 8, nz), F32),
            pltpu.VMEM((len(LO) + len(HI), 8, nz), F32),
            pltpu.VMEM((8, 8, 128), F32),
            pltpu.VMEM((8, 128), F32),
            pltpu.VMEM((3, 8, 128), F32),
            pltpu.VMEM((sizes["gx"], 8, 128), F32),
            pltpu.VMEM((sizes["gy"], 8, 128), F32),
            pltpu.VMEM((sizes["gz"], 8, 128), F32),
            pltpu.SemaphoreType.DMA((5,)),
            pltpu.SemaphoreType.DMA((24,)),
            pltpu.SemaphoreType.DMA((24,)),
            pltpu.SemaphoreType.DMA((peers,)),
            pltpu.SemaphoreType.DMA((peers,)),
        ],
        compiler_params=pltpu.CompilerParams(
            collective_id=0, has_side_effects=True, vmem_limit_bytes=60 * 2**20),
        name="krylov",
    )(rhs, stencil)

    step = 2
    block = pl.BlockSpec((nf, step, ny, nz), lambda i: (0, i, 0, 0))

    def last(*refs):
        final_kernel(ny // 8, step, *refs)

    return pl.pallas_call(
        last,
        grid=(nx // step,),
        out_shape=(field, field),
        in_specs=[pl.BlockSpec(memory_space=pltpu.SMEM), block, block, block],
        out_specs=(block, block),
        scratch_shapes=[pltpu.VMEM((2, 8, 8, 8, 128), F32)],
        compiler_params=pltpu.CompilerParams(dimension_semantics=("arbitrary",), vmem_limit_bytes=32 * 2**20),
        name="combine",
    )(c, rhs, q1, q2)


def solution(mesh):
    sizes = {a: mesh.shape[a] for a in AXES}
    spec = P(None, "gx", "gy", "gz")

    def run(rhs, stencil):
        return shards(sizes, rhs, stencil)

    return jax.shard_map(run, mesh=mesh, in_specs=(spec, spec), out_specs=(spec, spec), check_vma=False)
```

```python
import jax
import jax.numpy as jnp
from jax import lax
from jax.experimental import pallas as pl
from jax.experimental.pallas import tpu as pltpu
from jax.sharding import PartitionSpec as P

FORWARD = [
    (a, b, c) for a in (-1, 0, 1) for b in (-1, 0, 1) for c in (-1, 0, 1) if (a, b, c) > (0, 0, 0)
]
AXES = ("gx", "gy", "gz")
LO = [k for k, o in enumerate(FORWARD) if o[2] == 1]
HI = [k for k, o in enumerate(FORWARD) if o[2] == -1]
EX = [k for k, o in enumerate(FORWARD) if o[0] == 1]
F32 = jnp.float32


def runs(ks):
    out = []
    for k in ks:
        if out and out[-1][1] == k:
            out[-1][1] = k + 1
        else:
            out.append([k, k + 1])
    return out


def mm(a, b):
    total = a[:, 0:1] * b[0:1, :]
    for k in range(1, 8):
        total = total + a[:, k : k + 1] * b[k : k + 1, :]
    return total


def solve(matrix, right, row):
    aug = matrix + pltpu.roll(right, 8, 1)
    for k in range(8):
        pivot = aug[k : k + 1, :] / aug[k : k + 1, k : k + 1]
        aug = jnp.where(row == k, pivot, aug - aug[:, k : k + 1] * pivot)
    return pltpu.roll(aug, 120, 1)


def transposed(a, row, lane):
    out = jnp.zeros_like(a)
    for i in range(8):
        line = jnp.sum(jnp.where(lane == row, a[:, i : i + 1], 0.0), axis=0, keepdims=True)
        out = out + jnp.where(row == i, line, 0.0)
    return out


def main_kernel(sizes, dims, rhs, sten, q1_out, q2_out, c_out, p0, q0, pm, pp, w, ws, s0, diag, q2,
                zsend, zrecv, wzsend, wzrecv, red, gacc, cur, slot_x, slot_y, slot_z, lsem,
                xs, xr, ars, arr):
    nf, nx, ny = dims
    yb_n = ny // 8
    tall = ny + 16
    tiles = tall // 8
    pos = {a: lax.axis_index(a) for a in AXES}
    lane = lax.broadcasted_iota(jnp.int32, (8, 128), 1)
    row = lax.broadcasted_iota(jnp.int32, (8, 128), 0)
    ys = pl.ds(8, ny)

    loads = [
        pltpu.make_async_copy(rhs, p0.at[:, pl.ds(1, nx), ys], lsem.at[0]),
        pltpu.make_async_copy(sten.at[pl.ds(1, 13)], w.at[:, pl.ds(1, nx), ys], lsem.at[1]),
        pltpu.make_async_copy(sten.at[0], s0, lsem.at[2]),
    ]
    for copy in loads:
        copy.start()

    for buf in (p0, q0):
        for x in (0, nx + 1):
            buf[:, x] = jnp.zeros((nf, tall, 128), F32)
    w[:, 0] = jnp.zeros((13, tall, 128), F32)

    def clear(x, carry):
        for y in (0, ny + 8):
            p0[:, x, y : y + 8] = jnp.zeros((nf, 8, 128), F32)
            q0[:, x, y : y + 8] = jnp.zeros((nf, 8, 128), F32)
            w[:, x, y : y + 8] = jnp.zeros((13, 8, 128), F32)
        return carry

    lax.fori_loop(1, nx + 1, clear, 0)
    zrecv[...] = jnp.zeros(zrecv.shape, F32)
    wzrecv[...] = jnp.zeros(wzrecv.shape, F32)

    barrier = pltpu.get_barrier_semaphore()
    for a in AXES:
        for d in range(1, sizes[a]):
            pl.semaphore_signal(barrier, inc=1, device_id={a: lax.rem(pos[a] + d, sizes[a])},
                                device_id_type=pl.DeviceIdType.MESH)
    pl.semaphore_wait(barrier, sum(sizes[a] - 1 for a in AXES))

    count = [0]

    def shift(axis, up, src, dst):
        n = sizes[axis]
        i = pos[axis]
        slot = count[0]
        count[0] += 1
        copy = pltpu.make_async_remote_copy(
            src_ref=src, dst_ref=dst, send_sem=xs.at[slot], recv_sem=xr.at[slot],
            device_id={axis: lax.rem(i + (1 if up else n - 1), n)},
            device_id_type=pl.DeviceIdType.MESH)
        sends = i < n - 1 if up else i > 0
        gets = i > 0 if up else i < n - 1

        @pl.when(sends)
        def _():
            copy.start()

        def finish():
            @pl.when(sends)
            def _():
                copy.wait_send()

            @pl.when(gets)
            def _():
                copy.wait_recv()

        return finish

    def finish_all(items):
        for f in items:
            f()

    def y_faces(buf, start, length):
        xs_ = pl.ds(start, length)
        return [
            shift("gy", True, buf.at[:, xs_, pl.ds(ny, 8)], buf.at[:, xs_, pl.ds(0, 8)]),
            shift("gy", False, buf.at[:, xs_, pl.ds(8, 8)], buf.at[:, xs_, pl.ds(ny + 8, 8)]),
        ]

    def w_faces(start, length, edge):
        xs_ = pl.ds(start, length)
        out = []
        for b, up, src, dst in ((1, True, ny, 0), (-1, False, 8, ny + 8)):
            for lo, hi in runs([k for k, o in enumerate(FORWARD) if o[1] == b and (o[0] or not edge)]):
                ks = pl.ds(lo, hi - lo)
                out.append(shift("gy", up, w.at[ks, xs_, pl.ds(src, 8)], w.at[ks, xs_, pl.ds(dst, 8)]))
        return out

    OWN = (1, nx, 1)
    EDGE = (0, 2, nx + 1)
    W_EDGE = (0, 1, 1)

    def pack(part, take_low, take_high, n_low, n_high):
        first, depth, stride = part

        def body(t, accs):
            low, high = accs
            x = first + t * stride
            for yb in range(tiles):
                j = t * tiles + yb
                here = (lane == j)[None]
                low = jnp.where(here, pltpu.roll(take_low(x, yb), lax.rem(j + 1, 128), 2), low)
                high = jnp.where(here, pltpu.roll(take_high(x, yb), j, 2), high)
            return low, high

        return lax.fori_loop(0, depth, body,
                             (jnp.zeros((n_low, 8, 128), F32), jnp.zeros((n_high, 8, 128), F32)))

    def of(ks):
        def take(x, yb):
            return jnp.concatenate([w[k : k + 1, x, yb * 8 : yb * 8 + 8] for k in ks], axis=0)

        return take

    def gram(g, u, v):
        def body(x, accs):
            accs = list(accs)
            for yb in range(yb_n):
                ub = u(x, yb)
                vb = v(x, yb)
                for i in range(nf):
                    accs[i] = accs[i] + ub[i : i + 1] * vb[i:]
            return tuple(accs)

        accs = lax.fori_loop(0, nx, body, tuple(jnp.zeros((nf - i, 8, 128), F32) for i in range(nf)))
        red[...] = jnp.zeros(red.shape, F32)
        for i in range(nf):
            red[i, i:nf, :] = jnp.sum(accs[i], axis=1)
        out = jnp.zeros((8, 128), F32)
        for i in range(nf):
            t = jnp.sum(red[i], axis=1, keepdims=True)
            out = out + jnp.where(lane == 8 * g + i, t, 0.0)
            line = jnp.sum(jnp.where(lane == 8 * g + row, t, 0.0), axis=0, keepdims=True)
            out = out + jnp.where((row == i) & (lane > 8 * g + i), line, 0.0)
        if g == 0:
            gacc[...] = out
        else:
            gacc[...] += out

    def own(buf):
        return lambda x, yb: buf[:, x + 1, 8 + yb * 8 : 16 + yb * 8]

    def z_send(buf, e, part):
        p = 0 if part is OWN else 1

        def take(x, yb):
            return buf[:, x, yb * 8 : yb * 8 + 8]

        low, high = pack(part, take, take, nf, nf)
        zsend[e, p, 0] = low
        zsend[e, p, 1] = high
        return [
            shift("gz", True, zsend.at[e, p, 0], zrecv.at[e, p, 0]),
            shift("gz", False, zsend.at[e, p, 1], zrecv.at[e, p, 1]),
        ]

    def w_send(part):
        p = 0 if part is OWN else 1
        low, high = pack(part, of(LO), of(HI), len(LO), len(HI))
        wzsend[p, 0 : len(LO)] = low
        wzsend[p, len(LO) : len(LO) + len(HI)] = high
        lo_part, hi_part = pl.ds(0, len(LO)), pl.ds(len(LO), len(HI))
        return [
            shift("gz", True, wzsend.at[p, lo_part], wzrecv.at[p, lo_part]),
            shift("gz", False, wzsend.at[p, hi_part], wzrecv.at[p, hi_part]),
        ]

    def z_fill(buf, e, part):
        p = 0 if part is OWN else 1
        first, depth, stride = part

        def body(t, carry):
            x = first + t * stride
            for yb in range(tiles):
                j = t * tiles + yb
                v = buf[:, x, yb * 8 : yb * 8 + 8]
                low = pltpu.roll(zrecv[e, p, 0], lax.rem(128 - j, 128), 2)
                high = pltpu.roll(zrecv[e, p, 1], 127 - j, 2)
                pm[:, x, yb * 8 : yb * 8 + 8] = jnp.where((lane == 0)[None], low, pltpu.roll(v, 1, 2))
                pp[:, x, yb * 8 : yb * 8 + 8] = jnp.where((lane == 127)[None], high, pltpu.roll(v, 127, 2))
            return carry

        lax.fori_loop(0, depth, body, 0)

    def w_fill(part):
        p = 0 if part is OWN else 1
        first, depth, stride = part

        def body(t, carry):
            x = first + t * stride
            for yb in range(tiles):
                j = t * tiles + yb
                for n, k in enumerate(LO):
                    v = pltpu.roll(w[k, x, yb * 8 : yb * 8 + 8], 1, 1)
                    ws[k, x, yb * 8 : yb * 8 + 8] = jnp.where(
                        lane == 0, pltpu.roll(wzrecv[p, n], lax.rem(128 - j, 128), 1), v)
                for n, k in enumerate(HI):
                    v = pltpu.roll(w[k, x, yb * 8 : yb * 8 + 8], 127, 1)
                    ws[k, x, yb * 8 : yb * 8 + 8] = jnp.where(
                        lane == 127, pltpu.roll(wzrecv[p, len(LO) + n], 127 - j, 1), v)
            return carry

        lax.fori_loop(0, depth, body, 0)

    def behind(k, x, yb):
        a, b, c = FORWARD[k]
        src = w if c == 0 else ws
        return src[k, x + 1 - a, 8 + yb * 8 - b : 16 + yb * 8 - b]

    def ahead(k, x, yb):
        return w[k, x + 1, 8 + yb * 8 : 16 + yb * 8]

    def stencil(buf, put, first, depth, stride):
        views = {0: buf, -1: pm, 1: pp}

        def body(t, carry):
            x = first + t * stride
            for yb in range(yb_n):
                y = 8 + yb * 8
                acc = diag[x, yb * 8 : yb * 8 + 8][None] * buf[:, x + 1, y : y + 8]
                for k, (a, b, c) in enumerate(FORWARD):
                    acc = acc - ahead(k, x, yb)[None] * views[c][:, x + 1 + a, y + b : y + b + 8]
                    acc = acc - behind(k, x, yb)[None] * views[-c][:, x + 1 - a, y - b : y - b + 8]
                put(x, yb, acc)
            return carry

        lax.fori_loop(0, depth, body, 0)

    k0, k1 = EX[0], EX[-1] + 1
    phase = [
        shift("gx", True, rhs.at[:, nx - 1], p0.at[:, 0, ys]),
        shift("gx", False, rhs.at[:, 0], p0.at[:, nx + 1, ys]),
        shift("gx", True, sten.at[pl.ds(k0 + 1, k1 - k0), nx - 1], w.at[pl.ds(k0, k1 - k0), 0, ys]),
    ]
    def make_diag(x, carry):
        for yb in range(yb_n):
            total = s0[x, yb * 8 : yb * 8 + 8]
            for k in range(13):
                total = total + ahead(k, x, yb) + behind(k, x, yb)
            diag[x, yb * 8 : yb * 8 + 8] = total
        return carry

    def put_q1(x, yb, v):
        q0[:, x + 1, 8 + yb * 8 : 16 + yb * 8] = v

    def put_q2(x, yb, v):
        q2[:, x, yb * 8 : yb * 8 + 8] = v

    half = (nx - 2) // 2

    def operate(buf, e, put, crossing):
        finish_all(crossing)
        ends = y_faces(buf, 0, 1) + y_faces(buf, nx + 1, 1)
        if e == 0:
            ends += w_faces(0, 1, True)
        stencil(buf, put, 1, half, 1)
        finish_all(ends)
        ends = z_send(buf, e, EDGE)
        if e == 0:
            ends += w_send(W_EDGE)
        stencil(buf, put, 1 + half, nx - 2 - half, 1)
        finish_all(ends)
        z_fill(buf, e, EDGE)
        if e == 0:
            w_fill(W_EDGE)
            lax.fori_loop(0, 1, make_diag, 0)
        stencil(buf, put, 0, 2, nx - 1)

    loads[0].wait()
    sides = y_faces(p0, 1, nx)
    loads[1].wait()
    sides += w_faces(1, nx, False)
    gram(0, own(p0), own(p0))
    loads[2].wait()
    finish_all(sides)
    sides = z_send(p0, 0, OWN)
    sides += w_send(OWN)
    finish_all(sides)
    z_fill(p0, 0, OWN)
    w_fill(OWN)
    lax.fori_loop(1, nx, make_diag, 0)
    operate(p0, 0, put_q1, phase)

    sides = y_faces(q0, 1, nx)
    phase = [
        shift("gx", True, q0.at[:, nx, ys], q0.at[:, 0, ys]),
        shift("gx", False, q0.at[:, 1, ys], q0.at[:, nx + 1, ys]),
    ]
    save1 = pltpu.make_async_copy(q0.at[:, pl.ds(1, nx), ys], q1_out, lsem.at[3])
    save1.start()
    gram(1, own(p0), own(q0))
    finish_all(sides)
    sides = z_send(q0, 1, OWN)
    gram(2, own(q0), own(q0))
    finish_all(sides)
    z_fill(q0, 1, OWN)
    operate(q0, 1, put_q2, phase)
    save2 = pltpu.make_async_copy(q2, q2_out, lsem.at[4])
    save2.start()
    gram(3, own(q0), lambda x, yb: q2[:, x, yb * 8 : yb * 8 + 8])

    total = gacc[...]
    base = 0
    for stage, (a, slots) in enumerate(zip(("gy", "gx", "gz"), (slot_y, slot_x, slot_z))):
        n = sizes[a]
        i = pos[a]
        cur[stage] = total
        slots[i] = total
        copies = []
        for d in range(1, n):
            copies.append(pltpu.make_async_remote_copy(
                src_ref=cur.at[stage], dst_ref=slots.at[i],
                send_sem=ars.at[base + d - 1], recv_sem=arr.at[base + d - 1],
                device_id={a: lax.rem(i + d, n)}, device_id_type=pl.DeviceIdType.MESH))
        for copy in copies:
            copy.start()
        for d, copy in zip(range(1, n), copies):
            copy.wait_send()
            pltpu.make_async_remote_copy(
                src_ref=cur.at[stage], dst_ref=slots.at[lax.rem(i + n - d, n)],
                send_sem=ars.at[base + d - 1], recv_sem=arr.at[base + d - 1],
                device_id={a: lax.rem(i + d, n)}, device_id_type=pl.DeviceIdType.MESH).wait_recv()
        total = slots[0]
        for s in range(1, n):
            total = total + slots[s]
        base += n - 1

    small = lane < 8
    parts = [jnp.where(small, pltpu.roll(total, (128 - 8 * g) % 128, 1), 0.0) for g in range(4)]
    rr, pq, ss, tt = parts
    alpha = jnp.where(small, solve(pq, rr, row), 0.0)
    alpha_t = transposed(alpha, row, lane)
    alpha_t = jnp.where(small, alpha_t, 0.0)
    ssa = mm(ss, alpha)
    new = rr - mm(alpha_t, pq) - mm(pq, alpha) + mm(alpha_t, ssa)
    beta = jnp.where(small, solve(rr, new, row), 0.0)
    ib = beta + jnp.where(lane == row, 1.0, 0.0)
    ib_t = jnp.where(small, transposed(ib, row, lane), 0.0)
    curve = mm(ib_t, mm(pq, ib) - ssa) - mm(alpha_t, mm(ss, ib) - mm(tt, alpha))
    alpha1 = jnp.where(small, solve(curve, new, row), 0.0)
    c_out[0] = alpha + mm(ib, alpha1)
    c_out[1] = mm(alpha, alpha1)
    save1.wait()
    save2.wait()


def final_kernel(yb_n, xs_n, c, r0, q1, q2, sol, res, table):
    @pl.when(pl.program_id(0) == 0)
    def _():
        for n in range(2):
            for i in range(8):
                for j in range(8):
                    table[n, i, j] = jnp.full((8, 128), c[n, i, j], F32)

    def body(x, carry):
        for yb in range(yb_n):
            y = slice(yb * 8, yb * 8 + 8)
            s = jnp.zeros((8, 8, 128), F32)
            e = r0[:, x, y]
            for i in range(8):
                t1, t2 = table[0, i], table[1, i]
                a, b, d = r0[i, x, y][None], q1[i, x, y][None], q2[i, x, y][None]
                s = s + (t1 * a - t2 * b)
                e = e + (t2 * d - t1 * b)
            sol[:, x, y] = s
            res[:, x, y] = e
        return carry

    lax.fori_loop(0, xs_n, body, 0)


def shards(sizes, rhs, stencil):
    nf, nx, ny, nz = rhs.shape
    tall = ny + 16
    field = jax.ShapeDtypeStruct(rhs.shape, F32)
    anyspace = pl.BlockSpec(memory_space=pl.ANY)
    peers = sum(sizes[a] - 1 for a in AXES)
    padded = pltpu.VMEM((nf, nx + 2, tall, nz), F32)

    def kernel(*refs):
        main_kernel(sizes, (nf, nx, ny), *refs)

    q1, q2, c = pl.pallas_call(
        kernel,
        out_shape=(field, field, jax.ShapeDtypeStruct((2, 8, 128), F32)),
        in_specs=[anyspace, anyspace],
        out_specs=(anyspace, anyspace, pl.BlockSpec(memory_space=pltpu.VMEM)),
        scratch_shapes=[
            padded, padded, padded, padded,
            pltpu.VMEM((13, nx + 1, tall, nz), F32),
            pltpu.VMEM((13, nx + 1, tall, nz), F32),
            pltpu.VMEM((nx, ny, nz), F32),
            pltpu.VMEM((nx, ny, nz), F32),
            pltpu.VMEM((nf, nx, ny, nz), F32),
            pltpu.VMEM((2, 2, 2, nf, 8, nz), F32),
            pltpu.VMEM((2, 2, 2, nf, 8, nz), F32),
            pltpu.VMEM((2, len(LO) + len(HI), 8, nz), F32),
            pltpu.VMEM((2, len(LO) + len(HI), 8, nz), F32),
            pltpu.VMEM((8, 8, 128), F32),
            pltpu.VMEM((8, 128), F32),
            pltpu.VMEM((3, 8, 128), F32),
            pltpu.VMEM((sizes["gx"], 8, 128), F32),
            pltpu.VMEM((sizes["gy"], 8, 128), F32),
            pltpu.VMEM((sizes["gz"], 8, 128), F32),
            pltpu.SemaphoreType.DMA((5,)),
            pltpu.SemaphoreType.DMA((40,)),
            pltpu.SemaphoreType.DMA((40,)),
            pltpu.SemaphoreType.DMA((peers,)),
            pltpu.SemaphoreType.DMA((peers,)),
        ],
        compiler_params=pltpu.CompilerParams(
            collective_id=0, has_side_effects=True, vmem_limit_bytes=60 * 2**20),
        name="krylov",
    )(rhs, stencil)

    step = 2
    block = pl.BlockSpec((nf, step, ny, nz), lambda i: (0, i, 0, 0))

    def last(*refs):
        final_kernel(ny // 8, step, *refs)

    return pl.pallas_call(
        last,
        grid=(nx // step,),
        out_shape=(field, field),
        in_specs=[pl.BlockSpec(memory_space=pltpu.SMEM), block, block, block],
        out_specs=(block, block),
        scratch_shapes=[pltpu.VMEM((2, 8, 8, 8, 128), F32)],
        compiler_params=pltpu.CompilerParams(dimension_semantics=("arbitrary",), vmem_limit_bytes=60 * 2**20),
        name="combine",
    )(c, rhs, q1, q2)


def solution(mesh):
    sizes = {a: mesh.shape[a] for a in AXES}
    spec = P(None, "gx", "gy", "gz")

    def run(rhs, stencil):
        return shards(sizes, rhs, stencil)

    return jax.shard_map(run, mesh=mesh, in_specs=(spec, spec), out_specs=(spec, spec), check_vma=False)
```

```python
import jax
import jax.numpy as jnp
from jax import lax
from jax.experimental import pallas as pl
from jax.experimental.pallas import tpu as pltpu
from jax.sharding import PartitionSpec as P

FORWARD = [
    (a, b, c) for a in (-1, 0, 1) for b in (-1, 0, 1) for c in (-1, 0, 1) if (a, b, c) > (0, 0, 0)
]
AXES = ("gx", "gy", "gz")
LO = [k for k, o in enumerate(FORWARD) if o[2] == 1]
HI = [k for k, o in enumerate(FORWARD) if o[2] == -1]
EX = [k for k, o in enumerate(FORWARD) if o[0] == 1]
F32 = jnp.float32


def runs(ks):
    out = []
    for k in ks:
        if out and out[-1][1] == k:
            out[-1][1] = k + 1
        else:
            out.append([k, k + 1])
    return out


def mm(a, b):
    total = a[:, 0:1] * b[0:1, :]
    for k in range(1, 8):
        total = total + a[:, k : k + 1] * b[k : k + 1, :]
    return total


def solve(matrix, right, row):
    aug = matrix + pltpu.roll(right, 8, 1)
    for k in range(8):
        pivot = aug[k : k + 1, :] / aug[k : k + 1, k : k + 1]
        aug = jnp.where(row == k, pivot, aug - aug[:, k : k + 1] * pivot)
    return pltpu.roll(aug, 120, 1)


def transposed(a, row, lane):
    out = jnp.zeros_like(a)
    for i in range(8):
        line = jnp.sum(jnp.where(lane == row, a[:, i : i + 1], 0.0), axis=0, keepdims=True)
        out = out + jnp.where(row == i, line, 0.0)
    return out


def main_kernel(sizes, dims, rhs, sten, q1_out, q2_out, c_out, p0, q0, pm, pp, w, ws, s0, diag, q2,
                zsend, zrecv, wzsend, wzrecv, red, gacc, gsum, cur, slot_x, slot_y, slot_z, lsem,
                xs, xr, ars, arr):
    nf, nx, ny = dims
    yb_n = ny // 8
    tall = ny + 16
    tiles = tall // 8
    pos = {a: lax.axis_index(a) for a in AXES}
    lane = lax.broadcasted_iota(jnp.int32, (8, 128), 1)
    row = lax.broadcasted_iota(jnp.int32, (8, 128), 0)
    ys = pl.ds(8, ny)

    loads = [
        pltpu.make_async_copy(rhs, p0.at[:, pl.ds(1, nx), ys], lsem.at[0]),
        pltpu.make_async_copy(sten.at[pl.ds(1, 13)], w.at[:, pl.ds(1, nx), ys], lsem.at[1]),
        pltpu.make_async_copy(sten.at[0], s0, lsem.at[2]),
    ]
    for copy in loads:
        copy.start()

    for buf in (p0, q0):
        for x in (0, nx + 1):
            buf[:, x] = jnp.zeros((nf, tall, 128), F32)
    w[:, 0] = jnp.zeros((13, tall, 128), F32)

    def clear(x, carry):
        for y in (0, ny + 8):
            p0[:, x, y : y + 8] = jnp.zeros((nf, 8, 128), F32)
            q0[:, x, y : y + 8] = jnp.zeros((nf, 8, 128), F32)
            w[:, x, y : y + 8] = jnp.zeros((13, 8, 128), F32)
        return carry

    lax.fori_loop(1, nx + 1, clear, 0)
    zrecv[...] = jnp.zeros(zrecv.shape, F32)
    wzrecv[...] = jnp.zeros(wzrecv.shape, F32)

    barrier = pltpu.get_barrier_semaphore()
    for a in AXES:
        for d in range(1, sizes[a]):
            pl.semaphore_signal(barrier, inc=1, device_id={a: lax.rem(pos[a] + d, sizes[a])},
                                device_id_type=pl.DeviceIdType.MESH)
    pl.semaphore_wait(barrier, sum(sizes[a] - 1 for a in AXES))

    count = [0]

    def shift(axis, up, src, dst):
        n = sizes[axis]
        i = pos[axis]
        slot = count[0]
        count[0] += 1
        copy = pltpu.make_async_remote_copy(
            src_ref=src, dst_ref=dst, send_sem=xs.at[slot], recv_sem=xr.at[slot],
            device_id={axis: lax.rem(i + (1 if up else n - 1), n)},
            device_id_type=pl.DeviceIdType.MESH)
        sends = i < n - 1 if up else i > 0
        gets = i > 0 if up else i < n - 1

        @pl.when(sends)
        def _():
            copy.start()

        def finish():
            @pl.when(sends)
            def _():
                copy.wait_send()

            @pl.when(gets)
            def _():
                copy.wait_recv()

        return finish

    def finish_all(items):
        for f in items:
            f()

    def y_faces(buf, start, length):
        xs_ = pl.ds(start, length)
        return [
            shift("gy", True, buf.at[:, xs_, pl.ds(ny, 8)], buf.at[:, xs_, pl.ds(0, 8)]),
            shift("gy", False, buf.at[:, xs_, pl.ds(8, 8)], buf.at[:, xs_, pl.ds(ny + 8, 8)]),
        ]

    def w_faces(start, length, edge):
        xs_ = pl.ds(start, length)
        out = []
        for b, up, src, dst in ((1, True, ny, 0), (-1, False, 8, ny + 8)):
            for lo, hi in runs([k for k, o in enumerate(FORWARD) if o[1] == b and (o[0] or not edge)]):
                ks = pl.ds(lo, hi - lo)
                out.append(shift("gy", up, w.at[ks, xs_, pl.ds(src, 8)], w.at[ks, xs_, pl.ds(dst, 8)]))
        return out

    OWN = (1, nx, 1)
    EDGE = (0, 2, nx + 1)
    W_EDGE = (0, 1, 1)

    def pack(part, take_low, take_high, n_low, n_high):
        first, depth, stride = part

        def body(t, accs):
            low, high = accs
            x = first + t * stride
            for yb in range(tiles):
                j = t * tiles + yb
                here = (lane == j)[None]
                low = jnp.where(here, pltpu.roll(take_low(x, yb), lax.rem(j + 1, 128), 2), low)
                high = jnp.where(here, pltpu.roll(take_high(x, yb), j, 2), high)
            return low, high

        return lax.fori_loop(0, depth, body,
                             (jnp.zeros((n_low, 8, 128), F32), jnp.zeros((n_high, 8, 128), F32)))

    def of(ks):
        def take(x, yb):
            return jnp.concatenate([w[k : k + 1, x, yb * 8 : yb * 8 + 8] for k in ks], axis=0)

        return take

    def gram(g, u, v):
        def body(x, accs):
            accs = list(accs)
            for yb in range(yb_n):
                ub = u(x, yb)
                vb = v(x, yb)
                for i in range(nf):
                    accs[i] = accs[i] + ub[i : i + 1] * vb[i:]
            return tuple(accs)

        accs = lax.fori_loop(0, nx, body, tuple(jnp.zeros((nf - i, 8, 128), F32) for i in range(nf)))
        red[...] = jnp.zeros(red.shape, F32)
        for i in range(nf):
            red[i, i:nf, :] = jnp.sum(accs[i], axis=1)
        out = jnp.zeros((8, 128), F32)
        for i in range(nf):
            t = jnp.sum(red[i], axis=1, keepdims=True)
            out = out + jnp.where(lane == 8 * g + i, t, 0.0)
            line = jnp.sum(jnp.where(lane == 8 * g + row, t, 0.0), axis=0, keepdims=True)
            out = out + jnp.where((row == i) & (lane > 8 * g + i), line, 0.0)
        if g in (0, 3):
            gacc[...] = out
        else:
            gacc[...] += out

    def own(buf):
        return lambda x, yb: buf[:, x + 1, 8 + yb * 8 : 16 + yb * 8]

    def z_send(buf, e, part):
        p = 0 if part is OWN else 1

        def take(x, yb):
            return buf[:, x, yb * 8 : yb * 8 + 8]

        low, high = pack(part, take, take, nf, nf)
        zsend[e, p, 0] = low
        zsend[e, p, 1] = high
        return [
            shift("gz", True, zsend.at[e, p, 0], zrecv.at[e, p, 0]),
            shift("gz", False, zsend.at[e, p, 1], zrecv.at[e, p, 1]),
        ]

    def w_send(part):
        p = 0 if part is OWN else 1
        low, high = pack(part, of(LO), of(HI), len(LO), len(HI))
        wzsend[p, 0 : len(LO)] = low
        wzsend[p, len(LO) : len(LO) + len(HI)] = high
        lo_part, hi_part = pl.ds(0, len(LO)), pl.ds(len(LO), len(HI))
        return [
            shift("gz", True, wzsend.at[p, lo_part], wzrecv.at[p, lo_part]),
            shift("gz", False, wzsend.at[p, hi_part], wzrecv.at[p, hi_part]),
        ]

    def z_fill(buf, e, part):
        p = 0 if part is OWN else 1
        first, depth, stride = part

        def body(t, carry):
            x = first + t * stride
            for yb in range(tiles):
                j = t * tiles + yb
                v = buf[:, x, yb * 8 : yb * 8 + 8]
                low = pltpu.roll(zrecv[e, p, 0], lax.rem(128 - j, 128), 2)
                high = pltpu.roll(zrecv[e, p, 1], 127 - j, 2)
                pm[:, x, yb * 8 : yb * 8 + 8] = jnp.where((lane == 0)[None], low, pltpu.roll(v, 1, 2))
                pp[:, x, yb * 8 : yb * 8 + 8] = jnp.where((lane == 127)[None], high, pltpu.roll(v, 127, 2))
            return carry

        lax.fori_loop(0, depth, body, 0)

    def w_fill(part):
        p = 0 if part is OWN else 1
        first, depth, stride = part

        def body(t, carry):
            x = first + t * stride
            for yb in range(tiles):
                j = t * tiles + yb
                for n, k in enumerate(LO):
                    v = pltpu.roll(w[k, x, yb * 8 : yb * 8 + 8], 1, 1)
                    ws[k, x, yb * 8 : yb * 8 + 8] = jnp.where(
                        lane == 0, pltpu.roll(wzrecv[p, n], lax.rem(128 - j, 128), 1), v)
                for n, k in enumerate(HI):
                    v = pltpu.roll(w[k, x, yb * 8 : yb * 8 + 8], 127, 1)
                    ws[k, x, yb * 8 : yb * 8 + 8] = jnp.where(
                        lane == 127, pltpu.roll(wzrecv[p, len(LO) + n], 127 - j, 1), v)
            return carry

        lax.fori_loop(0, depth, body, 0)

    def behind(k, x, yb):
        a, b, c = FORWARD[k]
        src = w if c == 0 else ws
        return src[k, x + 1 - a, 8 + yb * 8 - b : 16 + yb * 8 - b]

    def ahead(k, x, yb):
        return w[k, x + 1, 8 + yb * 8 : 16 + yb * 8]

    def stencil(buf, put, first, depth, stride):
        views = {0: buf, -1: pm, 1: pp}

        def body(t, carry):
            x = first + t * stride
            for yb in range(yb_n):
                y = 8 + yb * 8
                acc = diag[x, yb * 8 : yb * 8 + 8][None] * buf[:, x + 1, y : y + 8]
                for k, (a, b, c) in enumerate(FORWARD):
                    acc = acc - ahead(k, x, yb)[None] * views[c][:, x + 1 + a, y + b : y + b + 8]
                    acc = acc - behind(k, x, yb)[None] * views[-c][:, x + 1 - a, y - b : y - b + 8]
                put(x, yb, acc)
            return carry

        lax.fori_loop(0, depth, body, 0)

    all_slots = (slot_y, slot_x, slot_z)
    bases = [0]
    for a in ("gy", "gx"):
        bases.append(bases[-1] + sizes[a] - 1)

    def sum_start(r, stage, value):
        a = ("gy", "gx", "gz")[stage]
        slots = all_slots[stage]
        n = sizes[a]
        i = pos[a]
        cur[r, stage] = value
        slots[r, i] = value

        def copy(d, dst):
            m = bases[stage] + d - 1
            return pltpu.make_async_remote_copy(
                src_ref=cur.at[r, stage], dst_ref=slots.at[r, dst],
                send_sem=ars.at[r, m], recv_sem=arr.at[r, m],
                device_id={a: lax.rem(i + d, n)}, device_id_type=pl.DeviceIdType.MESH)

        for d in range(1, n):
            copy(d, i).start()

        def finish():
            for d in range(1, n):
                copy(d, i).wait_send()
                copy(d, lax.rem(i + n - d, n)).wait_recv()
            total = slots[r, 0]
            for q in range(1, n):
                total = total + slots[r, q]
            return total

        return finish

    k0, k1 = EX[0], EX[-1] + 1
    phase = [
        shift("gx", True, rhs.at[:, nx - 1], p0.at[:, 0, ys]),
        shift("gx", False, rhs.at[:, 0], p0.at[:, nx + 1, ys]),
        shift("gx", True, sten.at[pl.ds(k0 + 1, k1 - k0), nx - 1], w.at[pl.ds(k0, k1 - k0), 0, ys]),
    ]
    def make_diag(x, carry):
        for yb in range(yb_n):
            total = s0[x, yb * 8 : yb * 8 + 8]
            for k in range(13):
                total = total + ahead(k, x, yb) + behind(k, x, yb)
            diag[x, yb * 8 : yb * 8 + 8] = total
        return carry

    def put_q1(x, yb, v):
        q0[:, x + 1, 8 + yb * 8 : 16 + yb * 8] = v

    def put_q2(x, yb, v):
        q2[:, x, yb * 8 : yb * 8 + 8] = v

    def stencil_pairs(buf, put, first, pairs):
        views = {0: buf, -1: pm, 1: pp}

        def body(t, carry):
            x = first + 2 * t
            for yb in range(yb_n):
                y = 8 + yb * 8
                accs = [None, None]
                for dx in (-1, 0, 1, 2):
                    for dy in (-1, 0, 1):
                        for dz in (-1, 0, 1):
                            v = views[dz][:, x + 1 + dx, y + dy : y + dy + 8]
                            for plane in (0, 1):
                                o = (dx - plane, dy, dz)
                                if abs(o[0]) > 1:
                                    continue
                                if o == (0, 0, 0):
                                    coef = -diag[x + plane, yb * 8 : yb * 8 + 8]
                                elif o > (0, 0, 0):
                                    coef = ahead(FORWARD.index(o), x + plane, yb)
                                else:
                                    back = (-o[0], -o[1], -o[2])
                                    coef = behind(FORWARD.index(back), x + plane, yb)
                                term = coef[None] * v
                                accs[plane] = -term if accs[plane] is None else accs[plane] - term
                for plane in (0, 1):
                    put(x + plane, yb, accs[plane])
            return carry

        lax.fori_loop(0, pairs, body, 0)

    half = (nx - 2) // 4

    def operate(buf, e, put, crossing, hooks=()):
        finish_all(crossing)
        ends = y_faces(buf, 0, 1) + y_faces(buf, nx + 1, 1)
        if e == 0:
            ends += w_faces(0, 1, True)
        stencil_pairs(buf, put, 1, half)
        if hooks:
            hooks[0]()
        finish_all(ends)
        ends = z_send(buf, e, EDGE)
        if e == 0:
            ends += w_send(W_EDGE)
        stencil_pairs(buf, put, 1 + 2 * half, (nx - 2) // 2 - half)
        if hooks:
            hooks[1]()
        finish_all(ends)
        z_fill(buf, e, EDGE)
        if e == 0:
            w_fill(W_EDGE)
            lax.fori_loop(0, 1, make_diag, 0)
        stencil(buf, put, 0, 2, nx - 1)

    loads[0].wait()
    sides = y_faces(p0, 1, nx)
    loads[1].wait()
    sides += w_faces(1, nx, False)
    gram(0, own(p0), own(p0))
    loads[2].wait()
    finish_all(sides)
    sides = z_send(p0, 0, OWN)
    sides += w_send(OWN)
    finish_all(sides)
    z_fill(p0, 0, OWN)
    w_fill(OWN)
    lax.fori_loop(1, nx, make_diag, 0)
    operate(p0, 0, put_q1, phase)

    sides = y_faces(q0, 1, nx)
    phase = [
        shift("gx", True, q0.at[:, nx, ys], q0.at[:, 0, ys]),
        shift("gx", False, q0.at[:, 1, ys], q0.at[:, nx + 1, ys]),
    ]
    save1 = pltpu.make_async_copy(q0.at[:, pl.ds(1, nx), ys], q1_out, lsem.at[3])
    save1.start()
    gram(1, own(p0), own(q0))
    finish_all(sides)
    sides = z_send(q0, 1, OWN)
    gram(2, own(q0), own(q0))
    pending = [sum_start(0, 0, gacc[...])]
    finish_all(sides)
    z_fill(q0, 1, OWN)
    pending.append(sum_start(0, 1, pending[0]()))

    def hook_a():
        pending.append(sum_start(0, 2, pending[1]()))

    def hook_b():
        gsum[...] = pending[2]()

    operate(q0, 1, put_q2, phase, (hook_a, hook_b))
    save2 = pltpu.make_async_copy(q2, q2_out, lsem.at[4])
    save2.start()
    gram(3, own(q0), lambda x, yb: q2[:, x, yb * 8 : yb * 8 + 8])

    done = sum_start(1, 0, gacc[...])
    total = gsum[...]
    small = lane < 8
    parts = [jnp.where(small, pltpu.roll(total, (128 - 8 * g) % 128, 1), 0.0) for g in range(3)]
    rr, pq, ss = parts
    alpha = jnp.where(small, solve(pq, rr, row), 0.0)
    done = sum_start(1, 1, done())
    alpha_t = transposed(alpha, row, lane)
    alpha_t = jnp.where(small, alpha_t, 0.0)
    ssa = mm(ss, alpha)
    new = rr - mm(alpha_t, pq) - mm(pq, alpha) + mm(alpha_t, ssa)
    beta = jnp.where(small, solve(rr, new, row), 0.0)
    done = sum_start(1, 2, done())
    ib = beta + jnp.where(lane == row, 1.0, 0.0)
    ib_t = jnp.where(small, transposed(ib, row, lane), 0.0)
    left = mm(ib_t, mm(pq, ib) - ssa)
    mid = mm(ss, ib)
    tt = jnp.where(small, pltpu.roll(done(), 128 - 24, 1), 0.0)
    curve = left - mm(alpha_t, mid - mm(tt, alpha))
    alpha1 = jnp.where(small, solve(curve, new, row), 0.0)
    c_out[0] = alpha + mm(ib, alpha1)
    c_out[1] = mm(alpha, alpha1)
    save1.wait()
    save2.wait()


def final_kernel(yb_n, xs_n, c, r0, q1, q2, sol, res, table):
    @pl.when(pl.program_id(0) == 0)
    def _():
        for n in range(2):
            for i in range(8):
                for j in range(8):
                    table[n, i, j] = jnp.full((8, 128), c[n, i, j], F32)

    def body(x, carry):
        for yb in range(yb_n):
            y = slice(yb * 8, yb * 8 + 8)
            s = jnp.zeros((8, 8, 128), F32)
            e = r0[:, x, y]
            for i in range(8):
                t1, t2 = table[0, i], table[1, i]
                a, b, d = r0[i, x, y][None], q1[i, x, y][None], q2[i, x, y][None]
                s = s + (t1 * a - t2 * b)
                e = e + (t2 * d - t1 * b)
            sol[:, x, y] = s
            res[:, x, y] = e
        return carry

    lax.fori_loop(0, xs_n, body, 0)


def shards(sizes, rhs, stencil):
    nf, nx, ny, nz = rhs.shape
    tall = ny + 16
    field = jax.ShapeDtypeStruct(rhs.shape, F32)
    anyspace = pl.BlockSpec(memory_space=pl.ANY)
    peers = sum(sizes[a] - 1 for a in AXES)
    padded = pltpu.VMEM((nf, nx + 2, tall, nz), F32)

    def kernel(*refs):
        main_kernel(sizes, (nf, nx, ny), *refs)

    q1, q2, c = pl.pallas_call(
        kernel,
        out_shape=(field, field, jax.ShapeDtypeStruct((2, 8, 128), F32)),
        in_specs=[anyspace, anyspace],
        out_specs=(anyspace, anyspace, pl.BlockSpec(memory_space=pltpu.VMEM)),
        scratch_shapes=[
            padded, padded, padded, padded,
            pltpu.VMEM((13, nx + 1, tall, nz), F32),
            pltpu.VMEM((13, nx + 1, tall, nz), F32),
            pltpu.VMEM((nx, ny, nz), F32),
            pltpu.VMEM((nx, ny, nz), F32),
            pltpu.VMEM((nf, nx, ny, nz), F32),
            pltpu.VMEM((2, 2, 2, nf, 8, nz), F32),
            pltpu.VMEM((2, 2, 2, nf, 8, nz), F32),
            pltpu.VMEM((2, len(LO) + len(HI), 8, nz), F32),
            pltpu.VMEM((2, len(LO) + len(HI), 8, nz), F32),
            pltpu.VMEM((8, 8, 128), F32),
            pltpu.VMEM((8, 128), F32),
            pltpu.VMEM((8, 128), F32),
            pltpu.VMEM((2, 3, 8, 128), F32),
            pltpu.VMEM((2, sizes["gx"], 8, 128), F32),
            pltpu.VMEM((2, sizes["gy"], 8, 128), F32),
            pltpu.VMEM((2, sizes["gz"], 8, 128), F32),
            pltpu.SemaphoreType.DMA((5,)),
            pltpu.SemaphoreType.DMA((40,)),
            pltpu.SemaphoreType.DMA((40,)),
            pltpu.SemaphoreType.DMA((2, peers)),
            pltpu.SemaphoreType.DMA((2, peers)),
        ],
        compiler_params=pltpu.CompilerParams(
            collective_id=0, has_side_effects=True, vmem_limit_bytes=60 * 2**20),
        name="krylov",
    )(rhs, stencil)

    step = 2
    block = pl.BlockSpec((nf, step, ny, nz), lambda i: (0, i, 0, 0))

    def last(*refs):
        final_kernel(ny // 8, step, *refs)

    return pl.pallas_call(
        last,
        grid=(nx // step,),
        out_shape=(field, field),
        in_specs=[pl.BlockSpec(memory_space=pltpu.SMEM), block, block, block],
        out_specs=(block, block),
        scratch_shapes=[pltpu.VMEM((2, 8, 8, 8, 128), F32)],
        compiler_params=pltpu.CompilerParams(dimension_semantics=("arbitrary",), vmem_limit_bytes=60 * 2**20),
        name="combine",
    )(c, rhs, q1, q2)


def solution(mesh):
    sizes = {a: mesh.shape[a] for a in AXES}
    spec = P(None, "gx", "gy", "gz")

    def run(rhs, stencil):
        return shards(sizes, rhs, stencil)

    return jax.shard_map(run, mesh=mesh, in_specs=(spec, spec), out_specs=(spec, spec), check_vma=False)
```
